32 devices in a mesh: freq: 2 (over x), leaf: 16 (over z, y, core).
Axes of the slice: x: 2, y: 2, z: 4, core: 2. Of those that a mesh axis runs over, the one named last changes fastest.
Arguments:
- rhs: float32 [128, 256, 128], P(('freq', 'leaf')), parts along dimension 0, may hold values from -6 to 6
- leaf_q: float32 [128, 256, 256], P(('freq', 'leaf')), parts along dimension 0, may hold values from -0.375 to 0.375
- leaf_e: float32 [128, 256, 256], P(('freq', 'leaf')), parts along dimension 0, may hold values from -0.375 to 0.375
- leaf_w: float32 [128, 256, 128], P(('freq', 'leaf')), parts along dimension 0, may hold values from -0.375 to 0.375
- node_q: float32 [96, 256, 256], P(('freq', 'leaf')), parts along dimension 0, may hold values from -0.375 to 0.375
- node_e: float32 [96, 256, 256], P(('freq', 'leaf')), parts along dimension 0, may hold values from -0.375 to 0.375
- node_w: float32 [96, 256, 128], P(('freq', 'leaf')), parts along dimension 0, may hold values from -0.375 to 0.375
- top_q: float32 [128, 256, 256], P(('freq', 'leaf')), parts along dimension 0, as said below
- top_e: float32 [128, 256, 256], P(('freq', 'leaf')), parts along dimension 0, as said below
- top_w: float32 [128, 256, 128], P(('freq', 'leaf')), parts along dimension 0, as said below
Outputs:
- solution: float32 [128, 256, 128], P(('freq', 'leaf')), parts along dimension 0
The draws below stay inside these ranges and needn't reach their ends.
There are 2 independent parts, one for each index of `freq`. The reference program is written for one: setup_inputs(seed, part) draws one part's arguments, and reference() takes and returns one part's arrays. A program takes and returns all parts, laid end to end along the dimension named above; each array names one. Nothing has to cross between parts.
Inputs may be any that keep to these rules, and one draw needn't show every extreme that they name: Device d's 4 rows of top_q hold, in row l-1, the transform of the level l node d // 2^l; devices with equal d // 2^l hold equal rows l-1. `top_e`: likewise for the inverted blocks: row l-1 of device d belongs to node d // 2^l of level l and is equal on all devices of that node. `top_w`: likewise for the generators: row l-1 of device d belongs to node d // 2^l of level l and is equal on all devices of that node.
All inputs are finite; a program needn't handle non-finite values.
Results may differ from the reference program's by a relative error of at most 0.00012.
Values sent between devices are 32-bit elements; how exact they have to be, the bound alone decides.
No kernel may reach another device: no remote copies, remote signals or barrier semaphores. Data moves between devices by JAX's collectives and lax.ppermute only.
A program may use at most 64 MiB of HBM per device.

```python
import jax
import jax.numpy as jnp
from jax import lax

M = 256
K = 128
R = 128
LEAF_DEV = 4
UPPER = 4
LEAVES = 64
N_LEAF = 16


def ancestors(key, salt, columns):
    blocks = []
    for level in range(1, UPPER + 1):
        count = N_LEAF // 2 ** level
        drawn = jax.random.normal(jax.random.fold_in(key, salt + level), (count, M, columns), jnp.float32) * M ** (-0.5)
        blocks.append(jnp.repeat(drawn, 2 ** level, axis=0))
    return jnp.stack(blocks, axis=1).reshape(N_LEAF * UPPER, M, columns)


def draw_top_q(key, part):
    return ancestors(key, 1000, M)


def draw_top_e(key, part):
    return ancestors(key, 2000, M)


def draw_top_w(key, part):
    return ancestors(key, 3000, K)


def levels(stream_key, extent, cuts, low, top_value):
    factor_of = 1.0
    for dim, parts in cuts:
        steps = jax.random.uniform(jax.random.fold_in(jax.random.fold_in(stream_key, 6), dim), (parts,), jnp.float32, low / len(cuts), top_value / len(cuts))
        factor_of = factor_of * jnp.repeat(jnp.exp(steps), extent[dim] // parts).reshape((-1,) + (1,) * (len(extent) - 1 - dim))
    return factor_of


def bell_draw(stream_key, shape, scale, limit, shards=(), kind=jnp.bfloat16):
    values = scale * jax.random.normal(stream_key, shape, jnp.float32)
    if shards:
        values = values * levels(stream_key, shape, shards, -0.22, 0.18)
    return jnp.clip(values, -limit, limit).astype(kind)


def setup_inputs(seed: int = 0, part: int = 0) -> dict:
    seeds = jax.random.split(jax.random.key(seed), 11)
    part_splits = jax.random.split(jax.random.fold_in(seeds[10], part), 11)
    rhs = bell_draw(part_splits[0], (LEAVES, M, R), 1.0, 6.0, ((0, 16),), jnp.float32)
    leaf_q = bell_draw(part_splits[1], (LEAVES, M, M), M ** -0.5, 0.375, ((0, 16),), jnp.float32)
    leaf_e = bell_draw(part_splits[2], (LEAVES, M, M), M ** -0.5, 0.375, ((0, 16),), jnp.float32)
    leaf_w = bell_draw(part_splits[3], (LEAVES, M, K), M ** -0.5, 0.375, ((0, 16),), jnp.float32)
    node_q = bell_draw(part_splits[4], (N_LEAF * (LEAF_DEV - 1), M, M), M ** -0.5, 0.375, ((0, 16),), jnp.float32)
    node_e = bell_draw(part_splits[5], (N_LEAF * (LEAF_DEV - 1), M, M), M ** -0.5, 0.375, ((0, 16),), jnp.float32)
    node_w = bell_draw(part_splits[6], (N_LEAF * (LEAF_DEV - 1), M, K), M ** -0.5, 0.375, ((0, 16),), jnp.float32)
    top_q = draw_top_q(jax.random.fold_in(jax.random.fold_in(seeds[10], part), 71), part)
    top_e = draw_top_e(jax.random.fold_in(jax.random.fold_in(seeds[10], part), 71), part)
    top_w = draw_top_w(jax.random.fold_in(jax.random.fold_in(seeds[10], part), 71), part)
    return dict(rhs=rhs, leaf_q=leaf_q, leaf_e=leaf_e, leaf_w=leaf_w, node_q=node_q, node_e=node_e, node_w=node_w, top_q=top_q, top_e=top_e, top_w=top_w)


HIGH = lax.Precision.HIGHEST


def batched(mats, vecs):
    return jnp.einsum("nij,njr->nir", mats, vecs, precision=HIGH)


def batched_t(mats, vecs):
    return jnp.einsum("nji,njr->nir", mats, vecs, precision=HIGH)


def upward(qmat, emat, wmat, vecs):
    values = batched(emat, batched(qmat, vecs))
    return values, batched_t(wmat, values)


def downward(qmat, emat, wmat, values, parent):
    return batched_t(qmat, values - batched(emat, batched(wmat, parent)))


def pick_level(gens, level):
    count = LEAF_DEV // 2 ** level
    offset = LEAF_DEV - 2 * count
    shaped = gens.reshape(N_LEAF, LEAF_DEV - 1, gens.shape[1], gens.shape[2])
    return shaped[:, offset:offset + count].reshape(-1, gens.shape[1], gens.shape[2])


def top_level(gens, level):
    shaped = gens.reshape(N_LEAF, UPPER, gens.shape[1], gens.shape[2])
    return shaped[::2 ** level, level - 1]


def reference(rhs, leaf_q, leaf_e, leaf_w, node_q, node_e, node_w, top_q, top_e, top_w):
    local_levels = LEAF_DEV.bit_length() - 1
    upper_levels = N_LEAF.bit_length() - 1
    width = leaf_w.shape[2]
    cols = rhs.shape[2]
    values, reduced = upward(leaf_q, leaf_e, leaf_w, rhs)
    local_values = [values]
    for level in range(1, local_levels + 1):
        stacked = reduced.reshape(-1, 2 * width, cols)
        values, reduced = upward(pick_level(node_q, level), pick_level(node_e, level), pick_level(node_w, level), stacked)
        local_values.append(values)
    upper_values = []
    for level in range(1, upper_levels + 1):
        stacked = reduced.reshape(-1, 2 * width, cols)
        values, reduced = upward(top_level(top_q, level), top_level(top_e, level), top_level(top_w, level), stacked)
        upper_values.append(values)
    answer = upper_values[-1]
    for level in range(upper_levels, 1, -1):
        parent = answer.reshape(-1, width, cols)
        answer = downward(top_level(top_q, level - 1), top_level(top_e, level - 1), top_level(top_w, level - 1), upper_values[level - 2], parent)
    parent = answer.reshape(-1, width, cols)
    for level in range(local_levels, 0, -1):
        answer = downward(pick_level(node_q, level), pick_level(node_e, level), pick_level(node_w, level), local_values[level], parent)
        parent = answer.reshape(-1, width, cols)
    return downward(leaf_q, leaf_e, leaf_w, local_values[0], parent)
```

```python
import functools

import jax
import jax.numpy as jnp
from jax import lax
from jax.experimental import pallas as pl
from jax.experimental.pallas import tpu as pltpu
from jax.sharding import PartitionSpec as P

F32 = jnp.float32
BF16 = jnp.bfloat16


def split(x):
    hi = x.astype(BF16)
    return hi, (x - hi.astype(F32)).astype(BF16)


def mul(a, b):
    left = jnp.concatenate([a[0], a[0], a[1]], axis=1)
    right = jnp.concatenate([b[0], b[1], b[0]], axis=0)
    return jnp.dot(left, right, preferred_element_type=F32)


def rows(pair, start, count):
    return pair[0][start : start + count], pair[1][start : start + count]


def beside(*pairs):
    return (
        jnp.concatenate([p[0] for p in pairs], axis=1),
        jnp.concatenate([p[1] for p in pairs], axis=1),
    )


def call(kernel, outs, ins, scratch=(), hbm_ins=()):
    specs = [
        pl.BlockSpec(memory_space=pltpu.HBM if i in hbm_ins else pltpu.VMEM)
        for i in range(len(ins))
    ]
    return pl.pallas_call(
        kernel,
        out_shape=[jax.ShapeDtypeStruct(s, d) for s, d in outs],
        in_specs=specs,
        out_specs=[pl.BlockSpec(memory_space=pltpu.VMEM) for _ in outs],
        scratch_shapes=list(scratch),
        compiler_params=pltpu.CompilerParams(vmem_limit_bytes=24 << 20),
    )(*[pltpu.with_memory_space_constraint(x, pltpu.HBM) if i in hbm_ins else x for i, x in enumerate(ins)])


def up_kernel(
    rhs, lq, le, lw, nq, ne, nw, tq, te, tw,
    c0, yl, yn, lqv, lev, lwv, nqv, nev, nwv, tqv, tev, twv,
    rhsv, sems,
):
    leaves = rhs.shape[0]
    nodes = nq.shape[0]
    width = lw.shape[2]
    copies = {}

    def start(name, src, dst):
        copy = pltpu.make_async_copy(src, dst, sems.at[len(copies)])
        copy.start()
        copies[name] = copy

    start("b", rhs, rhsv)
    for i in range(leaves):
        start(("q", i), lq.at[i], lqv.at[i])
    for i in range(leaves):
        start(("e", i), le.at[i], lev.at[i])
    start("w", lw, lwv)
    start("nq", nq, nqv)
    start("ne", ne, nev)
    start("nw", nw, nwv)
    start("tq", tq, tqv)
    start("te", te, tev)
    start("tw", tw, twv)

    copies["b"].wait()
    mid = []
    for i in range(leaves):
        copies["q", i].wait()
        mid.append(mul(split(lqv[i]), split(rhsv[i])))
    vals = []
    for i in range(leaves):
        copies["e", i].wait()
        y = mul(split(lev[i]), split(mid[i]))
        yl[i] = y
        vals.append(y)
    copies["w"].wait()
    reduced = [mul(split(lwv[i].T), split(vals[i])) for i in range(leaves)]
    copies["nq"].wait()
    copies["ne"].wait()
    copies["nw"].wait()
    offset = 0
    while len(reduced) > 1:
        count = len(reduced) // 2
        b = [jnp.concatenate(reduced[2 * j : 2 * j + 2], axis=0) for j in range(count)]
        t = [mul(split(nqv[offset + j]), split(b[j])) for j in range(count)]
        y = [mul(split(nev[offset + j]), split(t[j])) for j in range(count)]
        for j in range(count):
            yn[offset + j] = y[j]
        reduced = [mul(split(nwv[offset + j].T), split(y[j])) for j in range(count)]
        offset += count
    c0[...] = reduced[0]
    copies["tq"].wait()
    copies["te"].wait()
    copies["tw"].wait()


def side_of(level):
    position = lax.axis_index("leaf")
    return lax.rem(position // 2 ** (level - 1), 2)


def level_kernel(level, last, first, tq, te, tw, *refs):
    if first:
        t_in, outs = None, refs
    else:
        t_in, outs = refs[0], refs[1:]
    width = tw.shape[2]
    side = side_of(level)
    start = pl.multiple_of(side * width, width)
    q = split(tq[level - 1])
    if last:
        e_rows = split(te[level - 1, pl.ds(start, width), :])
        eq = mul(e_rows, q)
        if not first:
            eq = mul(split(t_in[...]), split(eq))
        outs[0][...] = eq
        return
    w = tw[level - 1]
    x = split(mul(split(te[level - 1]), beside(q, split(w))))
    q_half = tq[level - 1, :, pl.ds(start, width)]
    y = mul(split(jnp.concatenate([w.T, q_half.T], axis=0)), x)
    outs[0][:width] = y[:width, : 2 * width]
    low = y[width:]
    if not first:
        low = mul(split(t_in[...]), split(low))
    outs[0][width:] = low[:, : 2 * width]
    outs[1][...] = -low[:, 2 * width :]


def step_kernel(level, last, first, mat, own, other, *refs):
    if first:
        k_in, outs = None, refs
    else:
        k_in, outs = refs[0], refs[1:]
    width = own.shape[0]
    right = side_of(level) == 1
    a, b = own[...], other[...]
    both = jnp.concatenate(
        [jnp.where(right, b, a), jnp.where(right, a, b)], axis=0
    )
    out = mul(split(mat[...]), split(both))
    k = out if last else out[width:]
    if not first:
        k = k + k_in[...]
    if not last:
        outs[0][...] = out[:width]
    outs[-1][...] = k


def descent_kernel(q, e, w, y, after, out):
    for i in range(q.shape[0]):
        ew = mul(split(e[i]), split(w[i]))
        out[i] = mul(split(q[i].T), beside(split(y[i]), split(ew)))


def compose_kernel(nq, ne, nw, yn, leaf_maps, after, const, coef):
    width = nw.shape[2]
    nodes = nq.shape[0]
    maps = []
    for i in range(nodes):
        ew = mul(split(ne[i]), split(nw[i]))
        maps.append(mul(split(nq[i].T), beside(split(yn[i]), split(ew))))
    cols = yn.shape[2]
    top = maps[-1]
    parent = [jnp.concatenate([top[:, :cols], -top[:, cols:]], axis=1)]

    def below(vg, block):
        moved = mul(split(vg[:, cols:]), split(block))
        return jnp.concatenate([vg[:, :cols] - moved[:, :cols], -moved[:, cols:]], axis=1)

    count, offset = 1, nodes - 1
    while offset > 0:
        count *= 2
        offset -= count
        parent = [
            below(maps[offset + j], parent[j // 2][j % 2 * width : (j % 2 + 1) * width])
            for j in range(count)
        ]
    for i in range(leaf_maps.shape[0]):
        full = below(leaf_maps[i], parent[i // 2][i % 2 * width : (i % 2 + 1) * width])
        const[i] = full[:, :cols]
        coef[i] = full[:, cols:]


def final_kernel(level, mat, own, other, k, const, coef, out):
    width = own.shape[0]
    right = side_of(level) == 1
    a, b = own[...], other[...]
    both = jnp.concatenate(
        [jnp.where(right, b, a), jnp.where(right, a, b)], axis=0
    )
    g = split(mul(split(mat[...]), split(both)) + k[...])
    for i in range(out.shape[0]):
        out[i] = const[i] + mul(split(coef[i]), g)


def swapped(value, apart):
    pairs = [(i, i ^ 2**apart) for i in range(lax.axis_size("leaf"))]
    return lax.ppermute(value, "leaf", pairs)


def body(rhs, leaf_q, leaf_e, leaf_w, node_q, node_e, node_w, top_q, top_e, top_w):
    leaves, size, cols = rhs.shape
    nodes = node_q.shape[0]
    width = leaf_w.shape[2]
    levels = lax.axis_size("leaf").bit_length() - 1
    sq = (size, size)
    copies_of = [(a.shape, F32) for a in (leaf_q, leaf_e, leaf_w, node_q, node_e, node_w, top_q, top_e, top_w)]
    res = call(
        up_kernel,
        [((width, cols), F32), ((leaves, size, cols), F32), ((nodes, size, cols), F32)] + copies_of,
        [rhs, leaf_q, leaf_e, leaf_w, node_q, node_e, node_w, top_q, top_e, top_w],
        scratch=[pltpu.VMEM(rhs.shape, F32), pltpu.SemaphoreType.DMA((2 * leaves + 8,))],
        hbm_ins=range(10),
    )
    block, yl, yn, lq, le, lw, nq, ne, nw, tq, te, tw = res

    trans = []
    k = []
    leaf_maps = call(
        descent_kernel, [((leaves, size, cols + width), F32)], [lq, le, lw, yl, block]
    )[0]
    const, coef = call(
        compose_kernel,
        [((leaves, size, cols), F32), ((leaves, size, width), F32)],
        [nq, ne, nw, yn, leaf_maps, block],
    )
    for level in range(1, levels + 1):
        first, last = level == 1, level == levels
        other = swapped(block, level - 1)
        outs = [((width, size), F32)] if last else [((2 * width, size), F32), ((width, width), F32)]
        made = call(
            functools.partial(level_kernel, level, last, first), outs, [tq, te, tw] + trans
        )
        trans = list(made[1:])
        if last:
            return call(
                functools.partial(final_kernel, level),
                [((leaves, size, cols), F32)],
                [made[0], block, other, k[0], const, coef],
            )[0]
        block, k_new = call(
            functools.partial(step_kernel, level, last, first),
            [((width, cols), F32), ((width, cols), F32)],
            [made[0], block, other] + k,
        )
        k = [k_new]


def solution(mesh):
    spec = P(("freq", "leaf"), None, None)
    return jax.shard_map(body, mesh=mesh, in_specs=(spec,) * 10, out_specs=spec, check_vma=False)
```

```python
import functools

import jax
import jax.numpy as jnp
from jax import lax
from jax.experimental import pallas as pl
from jax.experimental.pallas import tpu as pltpu
from jax.sharding import PartitionSpec as P

F32 = jnp.float32
BF16 = jnp.bfloat16


def split(x):
    hi = x.astype(BF16)
    return hi, (x - hi.astype(F32)).astype(BF16)


def dot(a, b, contract=0):
    return lax.dot_general(a, b, (((1,), (contract,)), ((), ())), preferred_element_type=F32)


def mul(a, b):
    left = jnp.concatenate([a[0], a[0], a[1]], axis=1)
    right = jnp.concatenate([b[0], b[1], b[0]], axis=0)
    return dot(left, right)


def mul_narrow(a, b):
    m, n = a[0].shape[0], b[0].shape[1]
    r = dot(jnp.concatenate(a, axis=0), jnp.concatenate(b, axis=1))
    return r[:m, :n] + (r[:m, n:] + r[m:, :n])


def mul_short(a, b):
    m = a[0].shape[0]
    r = dot(jnp.concatenate(a, axis=0), b[0])
    return r[:m] + (r[m:] + dot(a[0], b[1]))


def beside(*pairs):
    return tuple(jnp.concatenate(parts, axis=1) for parts in zip(*pairs))


def call(kernel, outs, ins, scratch=(), hbm_ins=()):
    specs = [
        pl.BlockSpec(memory_space=pltpu.HBM if i in hbm_ins else pltpu.VMEM)
        for i in range(len(ins))
    ]
    ins = [
        pltpu.with_memory_space_constraint(x, pltpu.HBM) if i in hbm_ins else x
        for i, x in enumerate(ins)
    ]
    made = pl.pallas_call(
        kernel,
        out_shape=[jax.ShapeDtypeStruct(s, d) for s, d in outs],
        in_specs=specs,
        out_specs=[pl.BlockSpec(memory_space=pltpu.VMEM) for _ in outs],
        scratch_shapes=list(scratch),
        compiler_params=pltpu.CompilerParams(vmem_limit_bytes=24 << 20),
    )(*ins)
    return list(made)


def side_of(level):
    return lax.rem(lax.axis_index("leaf") // 2 ** (level - 1), 2)


def columns_of(levels):
    return lax.rem(sum(side_of(level) for level in range(1, levels + 1)), 2)


def up_kernel(
    levels, rhs, lq, le, lw, nq, ne, nw, tq, te, tw,
    keep, send, yl, bn, eqn, lqv, lev, lwv, nqv, nev, nwv, tqv, tev, twv,
    rhsv, sems,
):
    leaves, nodes = rhs.shape[0], nq.shape[0]
    copies = []

    def start(src, dst):
        copy = pltpu.make_async_copy(src, dst, sems.at[len(copies)])
        copy.start()
        copies.append(copy)
        return copy

    got_b = start(rhs, rhsv)
    got_q = [start(lq.at[i], lqv.at[i]) for i in range(leaves)]
    got_nq, got_ne = start(nq, nqv), start(ne, nev)
    got_e = [start(le.at[i], lev.at[i]) for i in range(leaves)]
    got_lw, got_nw = start(lw, lwv), start(nw, nwv)
    got_top = [start(tq, tqv), start(te, tev), start(tw, twv)]

    got_b.wait()
    mid, vals = [], []
    for i in range(0, leaves, 2):
        for j in (i, i + 1):
            got_q[j].wait()
        for j in (i, i + 1):
            mid.append(split(mul_narrow(split(lqv[j]), split(rhsv[j]))))
    got_nq.wait()
    got_ne.wait()
    eqs = []
    for i in range(nodes):
        eq = mul(split(nev[i]), split(nqv[i]))
        eqn[i] = eq
        eqs.append(split(eq))
    for i in range(0, leaves, 2):
        for j in (i, i + 1):
            got_e[j].wait()
        for j in (i, i + 1):
            y = mul_narrow(split(lev[j]), mid[j])
            yl[j] = y
            vals.append(split(y))
    got_lw.wait()
    got_nw.wait()
    maps = [split(mul(split(nwv[i].T), eqs[i])) for i in range(nodes)]
    reduced = [mul_narrow(split(lwv[i].T), vals[i]) for i in range(leaves)]
    offset = 0
    while len(reduced) > 1:
        count = len(reduced) // 2
        b = [jnp.concatenate(reduced[2 * j : 2 * j + 2], axis=0) for j in range(count)]
        for j in range(count):
            bn[offset + j] = b[j]
        reduced = [mul_narrow(maps[offset + j], split(b[j])) for j in range(count)]
        offset += count
    c = reduced[0].T
    half = c.shape[0] // 2
    low = columns_of(levels) == 0
    keep[...] = jnp.where(low, c[:half], c[half:])
    send[...] = jnp.where(low, c[half:], c[:half])
    for copy in got_top:
        copy.wait()


def level_kernel(level, levels, tq, te, tw, *refs):
    first, last = level == 1, level == levels
    outs = refs if first else refs[1:]
    width = tw.shape[2]
    half = pl.ds(pl.multiple_of(side_of(level) * width, width), width)
    at = level - 1
    if last:
        c = mul(split(te[at, half, :]), split(tq[at])).T
        if not first:
            c = mul(split(c), split(refs[0][...]))
        outs[0][...], outs[1][...] = split(c)
        return
    e, w = split(te[at]), split(tw[at])
    x = mul(e, split(tq[at]))
    z = mul_narrow(e, w)
    if first:
        q = split(tq[at])
        outs[0][...], outs[1][...] = split(mul(split(x.T), beside(w, q)))
        outs[2][...] = -mul(split(z.T), q)
        return
    q = split(tq[at, :, half])
    both = mul(split(x.T), beside(w, q))
    g = mul_narrow(split(z.T), q)
    low = mul(split(jnp.concatenate([both[:, width:], g], axis=0)), split(refs[0][...]))
    a = split(both[:, :width])
    tb = split(low[: 2 * width])
    for i in range(2):
        outs[i][:, :width] = a[i]
        outs[i][:, width:] = tb[i]
    outs[2][...] = -low[2 * width :]


def family(level, own, other):
    right = side_of(level) == 1
    a, b = own[...], other[...]
    return jnp.concatenate([jnp.where(right, b, a), jnp.where(right, a, b)], axis=1)


def step_kernel(level, hi, lo, own, other, *refs):
    width = own.shape[1]
    both = split(family(level, own, other))
    out = mul_short(both, (hi[...], lo[...]))
    k = out[:, width:]
    if level > 1:
        k = k + refs[0][...]
    refs[-2][...] = out[:, :width]
    refs[-1][...] = k


def root_kernel(level, hi, lo, own, other, *refs):
    width = own.shape[1]
    x = mul_short(split(family(level, own, other)), (hi[...], lo[...]))
    if level > 1:
        x = x + refs[0][...]
    right = side_of(1) == 1
    refs[-2][...] = jnp.where(right, x[:, width:], x[:, :width])
    refs[-1][...] = jnp.where(right, x[:, :width], x[:, width:])


def leaf_kernel(begin, q, e, w, y, after, out):
    for i in range(out.shape[0]):
        at = begin + i
        ew = mul_narrow(split(e[at]), split(w[at]))
        out[i] = mul(split(q[at].T), beside(split(y[at]), split(ew)))


def node_kernel(q, e, w, b, eq, after, out):
    for i in range(out.shape[0]):
        y = mul_narrow(split(eq[i]), split(b[i]))
        ew = mul_narrow(split(e[i]), split(w[i]))
        out[i] = mul(split(q[i].T), beside(split(y), split(ew)))


def compose_kernel(node_maps, maps_a, maps_b, after, const, coef):
    nodes = node_maps.shape[0]
    half = maps_a.shape[0]
    cols = const.shape[2]
    width = maps_a.shape[2] - cols
    top = node_maps[nodes - 1]
    parent = [jnp.concatenate([top[:, :cols], -top[:, cols:]], axis=1)]

    def below(vg, j):
        block = split(parent[j // 2][j % 2 * width : (j % 2 + 1) * width])
        moved = mul(split(vg[:, cols:]), block)
        return jnp.concatenate([vg[:, :cols] - moved[:, :cols], -moved[:, cols:]], axis=1)

    count, offset = 1, nodes - 1
    while offset > 0:
        count *= 2
        offset -= count
        parent = [below(node_maps[offset + j], j) for j in range(count)]
    for i in range(2 * half):
        full = below(maps_a[i] if i < half else maps_b[i - half], i)
        const[i] = full[:, :cols]
        coef[i] = jnp.concatenate(split(full[:, cols:]), axis=1)


def final_kernel(levels, own, other, const, coef, out):
    low = columns_of(levels) == 0
    a, b = own[...], other[...]
    hi, lo = split(
        jnp.concatenate([jnp.where(low, a, b), jnp.where(low, b, a)], axis=0)
    )
    cols = hi.shape[0]
    g = jnp.concatenate(
        [
            jnp.concatenate([hi, hi], axis=1),
            jnp.concatenate([lo, jnp.zeros_like(lo)], axis=1),
        ],
        axis=0,
    )
    for i in range(out.shape[0]):
        moved = dot(coef[i], g, 1)
        out[i] = const[i] + (moved[:, :cols] + moved[:, cols:])


def swapped(value, mask):
    pairs = [(i, i ^ mask) for i in range(lax.axis_size("leaf"))]
    return lax.ppermute(value, "leaf", pairs)


def body(rhs, leaf_q, leaf_e, leaf_w, node_q, node_e, node_w, top_q, top_e, top_w):
    leaves, size, cols = rhs.shape
    nodes = node_q.shape[0]
    width = leaf_w.shape[2]
    levels = lax.axis_size("leaf").bit_length() - 1
    weights = [leaf_q, leaf_e, leaf_w, node_q, node_e, node_w, top_q, top_e, top_w]
    res = call(
        functools.partial(up_kernel, levels),
        [
            ((cols // 2, width), F32),
            ((cols // 2, width), F32),
            (rhs.shape, F32),
            ((nodes, size, cols), F32),
            (node_q.shape, F32),
        ]
        + [(a.shape, F32) for a in weights],
        [rhs] + weights,
        scratch=[pltpu.VMEM(rhs.shape, F32), pltpu.SemaphoreType.DMA((2 * leaves + 8,))],
        hbm_ins=range(10),
    )
    block, sent, yl, bn, eqn, lq, le, lw, nq, ne, nw, tq, te, tw = res

    half = leaves // 2
    leaf_map = lambda begin, after: call(
        functools.partial(leaf_kernel, begin),
        [((half, size, cols + width), F32)],
        [lq, le, lw, yl, after],
    )
    trans, k, maps, done = [], [], [], []
    for level in range(1, levels + 1):
        last = level == levels
        other = swapped(sent if level == 1 else block, 2 ** (level - 1) | 1)
        wide = 2 * width if last else 3 * width
        outs = [((size, wide), BF16)] * 2 + ([] if last else [((width, size), F32)])
        made = call(
            functools.partial(level_kernel, level, levels), outs, [tq, te, tw] + trans
        )
        trans = list(made[2:])
        done = []
        if level == min(2, levels):
            done += leaf_map(0, block)
        if level == min(3, levels):
            done += leaf_map(half, block)
        maps += done
        if last:
            node_maps = call(
                node_kernel,
                [((nodes, size, cols + width), F32)],
                [nq, ne, nw, bn, eqn, block],
            )
            done += node_maps
        block, k_new = call(
            functools.partial(root_kernel if last else step_kernel, level),
            [((cols // 2, width), F32), ((cols // 2, width if last else size), F32)],
            [made[0], made[1], block, other] + k + done,
        )
        k = [k_new]
    other = swapped(k[0], 1)
    const, coef = call(
        compose_kernel,
        [((leaves, size, cols), F32), ((leaves, size, 2 * width), BF16)],
        node_maps + maps + [block],
    )
    return call(
        functools.partial(final_kernel, levels),
        [((leaves, size, cols), F32)],
        [block, other, const, coef],
    )[0]


def solution(mesh):
    spec = P(("freq", "leaf"), None, None)
    return jax.shard_map(body, mesh=mesh, in_specs=(spec,) * 10, out_specs=spec, check_vma=False)
```

```python
import functools

import jax
import jax.numpy as jnp
from jax import lax
from jax.experimental import pallas as pl
from jax.experimental.pallas import tpu as pltpu
from jax.sharding import PartitionSpec as P

F32 = jnp.float32
BF16 = jnp.bfloat16


def split(x):
    hi = x.astype(BF16)
    return hi, (x - hi.astype(F32)).astype(BF16)


def dot(a, b, contract=0):
    return lax.dot_general(a, b, (((1,), (contract,)), ((), ())), preferred_element_type=F32)


def mul(a, b):
    left = jnp.concatenate([a[0], a[0], a[1]], axis=1)
    right = jnp.concatenate([b[0], b[1], b[0]], axis=0)
    return dot(left, right)


def mul_narrow(a, b):
    m, n = a[0].shape[0], b[0].shape[1]
    step = 64
    stack = [part[i : i + step] for i in range(0, m, step) for part in a]
    r = dot(jnp.concatenate(stack, axis=0), jnp.concatenate(b, axis=1))
    out = []
    for i in range(0, 2 * m, 2 * step):
        top, low = r[i : i + step], r[i + step : i + 2 * step]
        out.append(top[:, :n] + (top[:, n:] + low[:, :n]))
    return jnp.concatenate(out, axis=0)


def mul_short(a, b):
    m = a[0].shape[0]
    r = dot(jnp.concatenate(a, axis=0), b[0])
    return r[:m] + (r[m:] + dot(a[0], b[1]))


def beside(*pairs):
    return tuple(jnp.concatenate(parts, axis=1) for parts in zip(*pairs))


def call(kernel, outs, ins, scratch=(), hbm_ins=()):
    specs = [
        pl.BlockSpec(memory_space=pltpu.HBM if i in hbm_ins else pltpu.VMEM)
        for i in range(len(ins))
    ]
    ins = [
        pltpu.with_memory_space_constraint(x, pltpu.HBM) if i in hbm_ins else x
        for i, x in enumerate(ins)
    ]
    made = pl.pallas_call(
        kernel,
        out_shape=[jax.ShapeDtypeStruct(s, d) for s, d in outs],
        in_specs=specs,
        out_specs=[pl.BlockSpec(memory_space=pltpu.VMEM) for _ in outs],
        scratch_shapes=list(scratch),
        compiler_params=pltpu.CompilerParams(vmem_limit_bytes=24 << 20),
    )(*ins)
    return list(made)


def side_of(level):
    return lax.rem(lax.axis_index("leaf") // 2 ** (level - 1), 2)


def columns_of(levels):
    return lax.rem(sum(side_of(level) for level in range(1, levels + 1)), 2)


def up_kernel(
    levels, rhs, lq, le, lw, nq, ne, nw, tq, te, tw,
    keep, send, yl, bn, lqv, lev, lwv, nqv, nev, nwv, tqv, tev, twv,
    rhsv, sems,
):
    leaves, nodes = rhs.shape[0], nq.shape[0]
    copies = []

    def start(src, dst):
        copy = pltpu.make_async_copy(src, dst, sems.at[len(copies)])
        copy.start()
        copies.append(copy)
        return copy

    got_b = start(rhs, rhsv)
    got_q = start(lq, lqv)
    got_e = start(le, lev)
    got_node = [start(nw, nwv), start(ne, nev), start(nq, nqv)]
    got_lw = start(lw, lwv)
    got_top = [start(tq, tqv), start(te, tev), start(tw, twv)]

    got_b.wait()
    got_q.wait()
    mid = [split(mul_narrow(split(lqv[i]), split(rhsv[i]))) for i in range(leaves)]
    got_e.wait()
    vals = []
    for i in range(leaves):
        y = mul_narrow(split(lev[i]), mid[i])
        yl[i] = y
        vals.append(split(y))
    for copy in got_node + [got_lw]:
        copy.wait()
    half_maps = [split(mul(split(nwv[i].T), split(nev[i]))) for i in range(nodes)]
    maps = [split(mul(half_maps[i], split(nqv[i]))) for i in range(nodes)]
    reduced = [mul_narrow(split(lwv[i].T), vals[i]) for i in range(leaves)]
    offset = 0
    while len(reduced) > 1:
        count = len(reduced) // 2
        b = [jnp.concatenate(reduced[2 * j : 2 * j + 2], axis=0) for j in range(count)]
        for j in range(count):
            bn[offset + j] = b[j]
        reduced = [mul_narrow(maps[offset + j], split(b[j])) for j in range(count)]
        offset += count
    c = reduced[0].T
    half = c.shape[0] // 2
    low = columns_of(levels) == 0
    keep[...] = jnp.where(low, c[:half], c[half:])
    send[...] = jnp.where(low, c[half:], c[:half])
    for copy in got_top:
        copy.wait()


def level_kernel(level, levels, tq, te, tw, *refs):
    first, last = level == 1, level == levels
    outs = refs if first else refs[1:]
    width = tw.shape[2]
    half = pl.ds(pl.multiple_of(side_of(level) * width, width), width)
    at = level - 1
    if last:
        c = mul(split(te[at, half, :]), split(tq[at])).T
        yield
        if not first:
            c = mul(split(c), split(refs[0][...]))
        outs[0][...], outs[1][...] = split(c)
        return
    e, w = split(te[at]), split(tw[at])
    x = mul(e, split(tq[at]))
    z = mul_narrow(e, w)
    yield
    if first:
        q = split(tq[at])
        outs[0][...], outs[1][...] = split(mul(split(x.T), beside(w, q)))
        outs[2][...] = -mul(split(z.T), q)
        return
    q = split(tq[at, :, half])
    both = mul(split(x.T), beside(w, q))
    g = mul_narrow(split(z.T), q)
    yield
    low = mul(split(jnp.concatenate([both[:, width:], g], axis=0)), split(refs[0][...]))
    a = split(both[:, :width])
    tb = split(low[: 2 * width])
    for i in range(2):
        outs[i][:, :width] = a[i]
        outs[i][:, width:] = tb[i]
    outs[2][...] = -low[2 * width :]


def family(level, own, other):
    right = side_of(level) == 1
    a, b = own[...], other[...]
    return jnp.concatenate([jnp.where(right, b, a), jnp.where(right, a, b)], axis=1)


def step_kernel(level, hi, lo, own, other, *refs):
    width = own.shape[1]
    both = split(family(level, own, other))
    out = mul_short(both, (hi[...], lo[...]))
    k = out[:, width:]
    if level > 1:
        k = k + refs[0][...]
    refs[-2][...] = out[:, :width]
    refs[-1][...] = k


def root_kernel(level, hi, lo, own, other, *refs):
    width = own.shape[1]
    x = mul_short(split(family(level, own, other)), (hi[...], lo[...]))
    if level > 1:
        x = x + refs[0][...]
    right = side_of(1) == 1
    refs[-2][...] = jnp.where(right, x[:, width:], x[:, :width])
    refs[-1][...] = jnp.where(right, x[:, :width], x[:, width:])


def leaf_kernel(begin, q, e, w, y, after, out):
    run = range(out.shape[0])
    ew = [split(mul_narrow(split(e[begin + i]), split(w[begin + i]))) for i in run]
    yield
    for i in run:
        out[i] = mul(split(q[begin + i].T), beside(split(y[begin + i]), ew[i]))


def node_kernel(begin, q, e, w, b, after, out):
    run = range(out.shape[0])
    t = [split(mul_narrow(split(q[begin + i]), split(b[begin + i]))) for i in run]
    yield
    y_ew = [split(mul(split(e[begin + i]), beside(t[i], split(w[begin + i])))) for i in run]
    yield
    for i in run:
        out[i] = mul(split(q[begin + i].T), y_ew[i])


def compose_kernel(maps_a, root_map, maps_b, node_maps, after, const, coef):
    nodes = node_maps.shape[0] + 1
    half = maps_a.shape[0]
    cols = const.shape[2]
    width = maps_a.shape[2] - cols
    top = root_map[0]
    parent = [jnp.concatenate([top[:, :cols], -top[:, cols:]], axis=1)]

    def below(vg, j):
        block = split(parent[j // 2][j % 2 * width : (j % 2 + 1) * width])
        moved = mul(split(vg[:, cols:]), block)
        return jnp.concatenate([vg[:, :cols] - moved[:, :cols], -moved[:, cols:]], axis=1)

    count, offset = 1, nodes - 1
    while offset > 0:
        count *= 2
        offset -= count
        parent = [below(node_maps[offset + j], j) for j in range(count)]
    for i in range(2 * half):
        full = below(maps_a[i] if i < half else maps_b[i - half], i)
        const[i] = full[:, :cols]
        coef[i] = jnp.concatenate(split(full[:, cols:]), axis=1)


def final_kernel(levels, own, other, const, coef, out):
    low = columns_of(levels) == 0
    a, b = own[...], other[...]
    hi, lo = split(
        jnp.concatenate([jnp.where(low, a, b), jnp.where(low, b, a)], axis=0)
    )
    cols = hi.shape[0]
    g = jnp.concatenate(
        [
            jnp.concatenate([hi, hi], axis=1),
            jnp.concatenate([lo, jnp.zeros_like(lo)], axis=1),
        ],
        axis=0,
    )
    for i in range(out.shape[0]):
        moved = dot(coef[i], g, 1)
        out[i] = const[i] + (moved[:, :cols] + moved[:, cols:])


def window_kernel(parts, *refs):
    taken = sum(n_in for _, n_in, _ in parts)
    given = taken
    at = 0
    running = []
    for part, n_in, n_out in parts:
        running.append(part(*refs[at : at + n_in], *refs[given : given + n_out]))
        at += n_in
        given += n_out
    while running:
        running = [job for job in running if next(job, True) is None]


def together(*jobs):
    parts = [(kernel, len(ins), len(outs)) for kernel, outs, ins in jobs]
    outs = [o for _, o, _ in jobs]
    flat = call(
        functools.partial(window_kernel, parts),
        sum(outs, []),
        sum([ins for _, _, ins in jobs], []),
    )
    results = []
    for o in outs:
        results.append(flat[: len(o)])
        flat = flat[len(o) :]
    return results


def swapped(value, mask):
    pairs = [(i, i ^ mask) for i in range(lax.axis_size("leaf"))]
    return lax.ppermute(value, "leaf", pairs)


def body(rhs, leaf_q, leaf_e, leaf_w, node_q, node_e, node_w, top_q, top_e, top_w):
    leaves, size, cols = rhs.shape
    nodes = node_q.shape[0]
    width = leaf_w.shape[2]
    levels = lax.axis_size("leaf").bit_length() - 1
    weights = [leaf_q, leaf_e, leaf_w, node_q, node_e, node_w, top_q, top_e, top_w]
    res = call(
        functools.partial(up_kernel, levels),
        [
            ((cols // 2, width), F32),
            ((cols // 2, width), F32),
            (rhs.shape, F32),
            ((nodes, size, cols), F32),
        ]
        + [(a.shape, F32) for a in weights],
        [rhs] + weights,
        scratch=[pltpu.VMEM(rhs.shape, F32), pltpu.SemaphoreType.DMA((10,))],
        hbm_ins=range(10),
    )
    block, sent, yl, bn, lq, le, lw, nq, ne, nw, tq, te, tw = res

    half = leaves // 2
    plan = {
        2: [(leaf_kernel, 0, half), (node_kernel, nodes - 1, 1)],
        3: [(leaf_kernel, half, half)],
        levels: [(node_kernel, 0, nodes - 1)],
    }
    trans, k, maps = [], [], []
    for level in range(1, levels + 1):
        last = level == levels
        other = swapped(sent if level == 1 else block, 2 ** (level - 1) | 1)
        wide = 2 * width if last else 3 * width
        jobs = [
            (
                functools.partial(level_kernel, level, levels),
                [((size, wide), BF16)] * 2 + ([] if last else [((width, size), F32)]),
                [tq, te, tw] + trans,
            )
        ]
        if level in plan:
            for kernel, begin, count in plan[level]:
                ins = [lq, le, lw, yl] if kernel is leaf_kernel else [nq, ne, nw, bn]
                jobs.append(
                    (
                        functools.partial(kernel, begin),
                        [((count, size, cols + width), F32)],
                        ins + [block],
                    )
                )
        made, *chores = together(*jobs)
        trans = made[2:]
        chores = [c[0] for c in chores]
        maps += chores
        block, k_new = call(
            functools.partial(root_kernel if last else step_kernel, level),
            [((cols // 2, width), F32), ((cols // 2, width if last else size), F32)],
            [made[0], made[1], block, other] + k + chores,
        )
        k = [k_new]
    other = swapped(k[0], 1)
    const, coef = call(
        compose_kernel,
        [((leaves, size, cols), F32), ((leaves, size, 2 * width), BF16)],
        maps + [block],
    )
    return call(
        functools.partial(final_kernel, levels),
        [((leaves, size, cols), F32)],
        [block, other, const, coef],
    )[0]


def solution(mesh):
    spec = P(("freq", "leaf"), None, None)
    return jax.shard_map(body, mesh=mesh, in_specs=(spec,) * 10, out_specs=spec, check_vma=False)
```

```python
import functools

import jax
import jax.numpy as jnp
from jax import lax
from jax.experimental import pallas as pl
from jax.experimental.pallas import tpu as pltpu
from jax.sharding import PartitionSpec as P

F32 = jnp.float32
BF16 = jnp.bfloat16


def split(x):
    hi = x.astype(BF16)
    return hi, (x - hi.astype(F32)).astype(BF16)


def dot(a, b, contract=0):
    return lax.dot_general(a, b, (((1,), (contract,)), ((), ())), preferred_element_type=F32)


def mul(a, b):
    left = jnp.concatenate([a[0], a[0], a[1]], axis=1)
    right = jnp.concatenate([b[0], b[1], b[0]], axis=0)
    return dot(left, right)


def mul_narrow(a, b):
    m, n = a[0].shape[0], b[0].shape[1]
    step = 64
    stack = [part[i : i + step] for i in range(0, m, step) for part in a]
    r = dot(jnp.concatenate(stack, axis=0), jnp.concatenate(b, axis=1))
    out = []
    for i in range(0, 2 * m, 2 * step):
        top, low = r[i : i + step], r[i + step : i + 2 * step]
        out.append(top[:, :n] + (top[:, n:] + low[:, :n]))
    return jnp.concatenate(out, axis=0)


def mul_short(a, b):
    m = a[0].shape[0]
    r = dot(jnp.concatenate(a, axis=0), b[0])
    return r[:m] + (r[m:] + dot(a[0], b[1]))


def beside(*pairs):
    return tuple(jnp.concatenate(parts, axis=1) for parts in zip(*pairs))


def call(kernel, outs, ins, scratch=(), hbm_ins=(), out_space=pltpu.VMEM):
    specs = [
        pl.BlockSpec(memory_space=pltpu.HBM if i in hbm_ins else pltpu.VMEM)
        for i in range(len(ins))
    ]
    ins = [
        pltpu.with_memory_space_constraint(x, pltpu.HBM) if i in hbm_ins else x
        for i, x in enumerate(ins)
    ]
    made = pl.pallas_call(
        kernel,
        out_shape=[jax.ShapeDtypeStruct(s, d) for s, d in outs],
        in_specs=specs,
        out_specs=[pl.BlockSpec(memory_space=out_space) for _ in outs],
        scratch_shapes=list(scratch),
        compiler_params=pltpu.CompilerParams(vmem_limit_bytes=24 << 20),
    )(*ins)
    return list(made)


def side_of(level):
    return lax.rem(lax.axis_index("leaf") // 2 ** (level - 1), 2)


def columns_of(levels):
    return lax.rem(sum(side_of(level) for level in range(1, levels + 1)), 2)


def up_kernel(
    levels, rhs, lq, le, lw, nq, ne, nw, tq, te, tw,
    keep, send, yl, bn, lqv, lev, lwv, nqv, nev, nwv, tqv, tev, twv,
    rhsv, sems,
):
    leaves, nodes = rhs.shape[0], nq.shape[0]
    copies = []

    def start(src, dst):
        copy = pltpu.make_async_copy(src, dst, sems.at[len(copies)])
        copy.start()
        copies.append(copy)
        return copy

    got_b = start(rhs, rhsv)
    got_q = start(lq, lqv)
    got_e = start(le, lev)
    got_node = [start(nw, nwv), start(ne, nev), start(nq, nqv)]
    got_lw = start(lw, lwv)
    got_top = [start(tq, tqv), start(te, tev), start(tw, twv)]

    got_b.wait()
    got_q.wait()
    mid = [split(mul_narrow(split(lqv[i]), split(rhsv[i]))) for i in range(leaves)]
    got_e.wait()
    vals = []
    for i in range(leaves):
        y = mul_narrow(split(lev[i]), mid[i])
        yl[i] = y
        vals.append(split(y))
    for copy in got_node + [got_lw]:
        copy.wait()
    half_maps = [split(mul(split(nwv[i].T), split(nev[i]))) for i in range(nodes)]
    reduced = [mul_narrow(split(lwv[i].T), vals[i]) for i in range(leaves)]
    maps = [split(mul(half_maps[i], split(nqv[i]))) for i in range(nodes)]
    offset = 0
    while len(reduced) > 1:
        count = len(reduced) // 2
        b = [jnp.concatenate(reduced[2 * j : 2 * j + 2], axis=0) for j in range(count)]
        for j in range(count):
            bn[offset + j] = b[j]
        reduced = [mul_narrow(maps[offset + j], split(b[j])) for j in range(count)]
        offset += count
    c = reduced[0].T
    half = c.shape[0] // 2
    low = columns_of(levels) == 0
    keep[...] = jnp.where(low, c[:half], c[half:])
    send[...] = jnp.where(low, c[half:], c[:half])
    for copy in got_top:
        copy.wait()


def level_kernel(level, levels, tq, te, tw, *refs):
    first, last = level == 1, level == levels
    outs = refs if first else refs[1:]
    width = tw.shape[2]
    half = pl.ds(pl.multiple_of(side_of(level) * width, width), width)
    at = level - 1
    if last:
        c = mul(split(te[at, half, :]), split(tq[at])).T
        yield
        if not first:
            c = mul(split(c), split(refs[0][...]))
        outs[0][...], outs[1][...] = split(c)
        return
    e, w = split(te[at]), split(tw[at])
    x = mul(e, split(tq[at]))
    z = mul_narrow(e, w)
    yield
    if first:
        q = split(tq[at])
        outs[0][...], outs[1][...] = split(mul(split(x.T), beside(w, q)))
        outs[2][...] = -mul(split(z.T), q)
        return
    q = split(tq[at, :, half])
    both = mul(split(x.T), beside(w, q))
    g = mul_narrow(split(z.T), q)
    yield
    low = mul(split(jnp.concatenate([both[:, width:], g], axis=0)), split(refs[0][...]))
    a = split(both[:, :width])
    tb = split(low[: 2 * width])
    for i in range(2):
        outs[i][:, :width] = a[i]
        outs[i][:, width:] = tb[i]
    outs[2][...] = -low[2 * width :]


def family(level, own, other):
    right = side_of(level) == 1
    a, b = own[...], other[...]
    return jnp.concatenate([jnp.where(right, b, a), jnp.where(right, a, b)], axis=1)


def step_kernel(level, hi, lo, own, other, *refs):
    width = own.shape[1]
    both = split(family(level, own, other))
    out = mul_short(both, (hi[...], lo[...]))
    k = out[:, width:]
    if level > 1:
        k = k + refs[0][...]
    refs[-2][...] = out[:, :width]
    refs[-1][...] = k


def root_kernel(level, hi, lo, own, other, *refs):
    width = own.shape[1]
    x = mul_short(split(family(level, own, other)), (hi[...], lo[...]))
    if level > 1:
        x = x + refs[0][...]
    right = side_of(1) == 1
    refs[-2][...] = jnp.where(right, x[:, width:], x[:, :width])
    refs[-1][...] = jnp.where(right, x[:, :width], x[:, width:])


def leaf_kernel(begin, q, e, w, y, after, out):
    run = range(out.shape[0])
    ew = [split(mul_narrow(split(e[begin + i]), split(w[begin + i]))) for i in run]
    yield
    for i in run:
        out[i] = mul(split(q[begin + i].T), beside(split(y[begin + i]), ew[i]))


def node_kernel(begin, q, e, w, b, after, out):
    run = range(out.shape[0])
    t = [split(mul_narrow(split(q[begin + i]), split(b[begin + i]))) for i in run]
    yield
    y_ew = [split(mul(split(e[begin + i]), beside(t[i], split(w[begin + i])))) for i in run]
    yield
    for i in run:
        out[i] = mul(split(q[begin + i].T), y_ew[i])


def compose_kernel(maps_a, root_map, maps_b, node_maps, after, const, coef):
    nodes = node_maps.shape[0] + 1
    half = maps_a.shape[0]
    cols = const.shape[2]
    width = maps_a.shape[2] - cols
    top = root_map[0]
    parent = [jnp.concatenate([top[:, :cols], -top[:, cols:]], axis=1)]

    def below(vg, j):
        block = split(parent[j // 2][j % 2 * width : (j % 2 + 1) * width])
        moved = mul(split(vg[:, cols:]), block)
        return jnp.concatenate([vg[:, :cols] - moved[:, :cols], -moved[:, cols:]], axis=1)

    count, offset = 1, nodes - 1
    while offset > 0:
        count *= 2
        offset -= count
        parent = [below(node_maps[offset + j], j) for j in range(count)]
    for i in range(2 * half):
        full = below(maps_a[i] if i < half else maps_b[i - half], i)
        const[i] = full[:, :cols]
        coef[i] = jnp.concatenate(split(full[:, cols:]), axis=1)


def final_kernel(levels, own, other, const, coef, out, held, sems):
    low = columns_of(levels) == 0
    a, b = own[...], other[...]
    hi, lo = split(
        jnp.concatenate([jnp.where(low, a, b), jnp.where(low, b, a)], axis=0)
    )
    cols = hi.shape[0]
    g = jnp.concatenate(
        [
            jnp.concatenate([hi, hi], axis=1),
            jnp.concatenate([lo, jnp.zeros_like(lo)], axis=1),
        ],
        axis=0,
    )
    copies = []
    for i in range(out.shape[0]):
        moved = dot(coef[i], g, 1)
        held[i] = const[i] + (moved[:, :cols] + moved[:, cols:])
        copies.append(pltpu.make_async_copy(held.at[i], out.at[i], sems.at[i]))
        copies[i].start()
    for copy in copies:
        copy.wait()


def window_kernel(parts, *refs):
    taken = sum(n_in for _, n_in, _ in parts)
    given = taken
    at = 0
    running = []
    for part, n_in, n_out in parts:
        running.append(part(*refs[at : at + n_in], *refs[given : given + n_out]))
        at += n_in
        given += n_out
    while running:
        running = [job for job in running if next(job, True) is None]


def together(*jobs):
    parts = [(kernel, len(ins), len(outs)) for kernel, outs, ins in jobs]
    outs = [o for _, o, _ in jobs]
    flat = call(
        functools.partial(window_kernel, parts),
        sum(outs, []),
        sum([ins for _, _, ins in jobs], []),
    )
    results = []
    for o in outs:
        results.append(flat[: len(o)])
        flat = flat[len(o) :]
    return results


def swapped(value, mask):
    pairs = [(i, i ^ mask) for i in range(lax.axis_size("leaf"))]
    return lax.ppermute(value, "leaf", pairs)


def body(rhs, leaf_q, leaf_e, leaf_w, node_q, node_e, node_w, top_q, top_e, top_w):
    leaves, size, cols = rhs.shape
    nodes = node_q.shape[0]
    width = leaf_w.shape[2]
    levels = lax.axis_size("leaf").bit_length() - 1
    weights = [leaf_q, leaf_e, leaf_w, node_q, node_e, node_w, top_q, top_e, top_w]
    res = call(
        functools.partial(up_kernel, levels),
        [
            ((cols // 2, width), F32),
            ((cols // 2, width), F32),
            (rhs.shape, F32),
            ((nodes, size, cols), F32),
        ]
        + [(a.shape, F32) for a in weights],
        [rhs] + weights,
        scratch=[pltpu.VMEM(rhs.shape, F32), pltpu.SemaphoreType.DMA((10,))],
        hbm_ins=range(10),
    )
    block, sent, yl, bn, lq, le, lw, nq, ne, nw, tq, te, tw = res

    half = leaves // 2
    plan = {
        2: [(leaf_kernel, 0, half), (node_kernel, nodes - 1, 1)],
        3: [(leaf_kernel, half, half)],
        levels: [(node_kernel, 0, nodes - 1)],
    }
    trans, k, maps = [], [], []
    for level in range(1, levels + 1):
        last = level == levels
        other = swapped(sent if level == 1 else block, 2 ** (level - 1) | 1)
        wide = 2 * width if last else 3 * width
        jobs = [
            (
                functools.partial(level_kernel, level, levels),
                [((size, wide), BF16)] * 2 + ([] if last else [((width, size), F32)]),
                [tq, te, tw] + trans,
            )
        ]
        if level in plan:
            for kernel, begin, count in plan[level]:
                ins = [lq, le, lw, yl] if kernel is leaf_kernel else [nq, ne, nw, bn]
                jobs.append(
                    (
                        functools.partial(kernel, begin),
                        [((count, size, cols + width), F32)],
                        ins + [block],
                    )
                )
        made, *chores = together(*jobs)
        trans = made[2:]
        chores = [c[0] for c in chores]
        maps += chores
        block, k_new = call(
            functools.partial(root_kernel if last else step_kernel, level),
            [((cols // 2, width), F32), ((cols // 2, width if last else size), F32)],
            [made[0], made[1], block, other] + k + chores,
        )
        k = [k_new]
    other = swapped(k[0], 1)
    const, coef = call(
        compose_kernel,
        [((leaves, size, cols), F32), ((leaves, size, 2 * width), BF16)],
        maps + [block],
    )
    return call(
        functools.partial(final_kernel, levels),
        [((leaves, size, cols), F32)],
        [block, other, const, coef],
        scratch=[pltpu.VMEM(rhs.shape, F32), pltpu.SemaphoreType.DMA((leaves,))],
        out_space=pltpu.HBM,
    )[0]


def solution(mesh):
    spec = P(("freq", "leaf"), None, None)
    return jax.shard_map(body, mesh=mesh, in_specs=(spec,) * 10, out_specs=spec, check_vma=False)
```

```python
import functools

import jax
import jax.numpy as jnp
from jax import lax
from jax.experimental import pallas as pl
from jax.experimental.pallas import tpu as pltpu
from jax.sharding import PartitionSpec as P

F32 = jnp.float32
BF16 = jnp.bfloat16


def split(x):
    hi = x.astype(BF16)
    return hi, (x - hi.astype(F32)).astype(BF16)


def dot(a, b, contract=0):
    return lax.dot_general(a, b, (((1,), (contract,)), ((), ())), preferred_element_type=F32)


def mul(a, b):
    left = jnp.concatenate([a[0], a[0], a[1]], axis=1)
    right = jnp.concatenate([b[0], b[1], b[0]], axis=0)
    return dot(left, right)


def mul_narrow(a, b):
    m, n = a[0].shape[0], b[0].shape[1]
    step = 64
    stack = [part[i : i + step] for i in range(0, m, step) for part in a]
    r = dot(jnp.concatenate(stack, axis=0), jnp.concatenate(b, axis=1))
    out = []
    for i in range(0, 2 * m, 2 * step):
        top, low = r[i : i + step], r[i + step : i + 2 * step]
        out.append(top[:, :n] + (top[:, n:] + low[:, :n]))
    return jnp.concatenate(out, axis=0)


def mul_short(a, b):
    m = a[0].shape[0]
    r = dot(jnp.concatenate(a, axis=0), b[0])
    return r[:m] + (r[m:] + dot(a[0], b[1]))


def beside(*pairs):
    return tuple(jnp.concatenate(parts, axis=1) for parts in zip(*pairs))


def call(kernel, outs, ins, scratch=(), hbm_ins=(), out_space=pltpu.VMEM):
    specs = [
        pl.BlockSpec(memory_space=pltpu.HBM if i in hbm_ins else pltpu.VMEM)
        for i in range(len(ins))
    ]
    ins = [
        pltpu.with_memory_space_constraint(x, pltpu.HBM) if i in hbm_ins else x
        for i, x in enumerate(ins)
    ]
    made = pl.pallas_call(
        kernel,
        out_shape=[jax.ShapeDtypeStruct(s, d) for s, d in outs],
        in_specs=specs,
        out_specs=[pl.BlockSpec(memory_space=out_space) for _ in outs],
        scratch_shapes=list(scratch),
        compiler_params=pltpu.CompilerParams(vmem_limit_bytes=24 << 20),
    )(*ins)
    return list(made)


def side_of(level):
    return lax.rem(lax.axis_index("leaf") // 2 ** (level - 1), 2)


def columns_of(levels):
    return lax.rem(sum(side_of(level) for level in range(1, levels + 1)), 2)


def up_kernel(
    levels, rhs, lq, le, lw, nq, ne, nw, tq, te, tw,
    keep, send, yl, bn, lqv, lev, lwv, nqv, nev, nwv, tqv, tev, twv,
    rhsv, sems,
):
    leaves, nodes = rhs.shape[0], nq.shape[0]
    copies = []

    def start(src, dst):
        copy = pltpu.make_async_copy(src, dst, sems.at[len(copies)])
        copy.start()
        copies.append(copy)
        return copy

    got = {}
    got['b'] = start(rhs, rhsv)
    got['q'] = start(lq, lqv)
    got['nw'] = start(nw, nwv)
    got['w'] = start(lw, lwv)
    got['e'] = start(le, lev)
    got['ne'] = start(ne, nev)
    got['nq'] = start(nq, nqv)
    got_top = [start(tq, tqv), start(te, tev), start(tw, twv)]

    got['b'].wait()
    got['q'].wait()
    mid = [split(mul_narrow(split(lqv[i]), split(rhsv[i]))) for i in range(leaves)]
    got['nw'].wait()
    got['w'].wait()
    got['e'].wait()
    vals = []
    for i in range(leaves):
        y = mul_narrow(split(lev[i]), mid[i])
        yl[i] = y
        vals.append(split(y))
    node_wt = [split(nwv[i].T) for i in range(nodes)]
    leaf_wt = [split(lwv[i].T) for i in range(leaves)]
    got['ne'].wait()
    got['nq'].wait()
    half_maps = [split(mul(node_wt[i], split(nev[i]))) for i in range(nodes)]
    reduced = [mul_narrow(leaf_wt[i], vals[i]) for i in range(leaves)]
    maps = [split(mul(half_maps[i], split(nqv[i]))) for i in range(nodes)]
    offset = 0
    while len(reduced) > 1:
        count = len(reduced) // 2
        b = [jnp.concatenate(reduced[2 * j : 2 * j + 2], axis=0) for j in range(count)]
        for j in range(count):
            bn[offset + j] = b[j]
        reduced = [mul_narrow(maps[offset + j], split(b[j])) for j in range(count)]
        offset += count
    c = reduced[0].T
    half = c.shape[0] // 2
    low = columns_of(levels) == 0
    keep[...] = jnp.where(low, c[:half], c[half:])
    send[...] = jnp.where(low, c[half:], c[:half])
    for copy in got_top:
        copy.wait()


def level_kernel(level, levels, tq, te, tw, *refs):
    first, last = level == 1, level == levels
    outs = refs if first else refs[1:]
    width = tw.shape[2]
    half = pl.ds(pl.multiple_of(side_of(level) * width, width), width)
    at = level - 1
    if last:
        c = mul(split(te[at, half, :]), split(tq[at])).T
        yield
        if not first:
            c = mul(split(c), split(refs[0][...]))
        outs[0][...], outs[1][...] = split(c)
        return
    e, w = split(te[at]), split(tw[at])
    x = mul(e, split(tq[at]))
    z = mul_narrow(e, w)
    yield
    if first:
        q = split(tq[at])
        outs[0][...], outs[1][...] = split(mul(split(x.T), beside(w, q)))
        outs[2][...] = -mul(split(z.T), q)
        return
    q = split(tq[at, :, half])
    both = mul(split(x.T), beside(w, q))
    g = mul_narrow(split(z.T), q)
    yield
    low = mul(split(jnp.concatenate([both[:, width:], g], axis=0)), split(refs[0][...]))
    a = split(both[:, :width])
    tb = split(low[: 2 * width])
    for i in range(2):
        outs[i][:, :width] = a[i]
        outs[i][:, width:] = tb[i]
    outs[2][...] = -low[2 * width :]


def family(level, own, other):
    right = side_of(level) == 1
    a, b = own[...], other[...]
    return jnp.concatenate([jnp.where(right, b, a), jnp.where(right, a, b)], axis=1)


def step_kernel(level, hi, lo, own, other, *refs):
    width = own.shape[1]
    both = split(family(level, own, other))
    out = mul_short(both, (hi[...], lo[...]))
    k = out[:, width:]
    if level > 1:
        k = k + refs[0][...]
    refs[-2][...] = out[:, :width]
    refs[-1][...] = k


def root_kernel(level, hi, lo, own, other, *refs):
    width = own.shape[1]
    x = mul_short(split(family(level, own, other)), (hi[...], lo[...]))
    if level > 1:
        x = x + refs[0][...]
    right = side_of(1) == 1
    refs[-2][...] = jnp.where(right, x[:, width:], x[:, :width])
    refs[-1][...] = jnp.where(right, x[:, :width], x[:, width:])


def leaf_kernel(begin, q, e, w, y, after, out):
    run = range(out.shape[0])
    ew = [split(mul_narrow(split(e[begin + i]), split(w[begin + i]))) for i in run]
    yield
    for i in run:
        out[i] = mul(split(q[begin + i].T), beside(split(y[begin + i]), ew[i]))


def node_kernel(begin, q, e, w, b, after, out):
    run = range(out.shape[0])
    t = [split(mul_narrow(split(q[begin + i]), split(b[begin + i]))) for i in run]
    yield
    y_ew = [split(mul(split(e[begin + i]), beside(t[i], split(w[begin + i])))) for i in run]
    yield
    for i in run:
        out[i] = mul(split(q[begin + i].T), y_ew[i])


def compose_kernel(maps_a, root_map, maps_b, node_maps, after, const, coef):
    nodes = node_maps.shape[0] + 1
    half = maps_a.shape[0]
    cols = const.shape[2]
    width = maps_a.shape[2] - cols
    top = root_map[0]
    parent = [jnp.concatenate([top[:, :cols], -top[:, cols:]], axis=1)]

    def below(vg, j):
        block = split(parent[j // 2][j % 2 * width : (j % 2 + 1) * width])
        moved = mul(split(vg[:, cols:]), block)
        return jnp.concatenate([vg[:, :cols] - moved[:, :cols], -moved[:, cols:]], axis=1)

    count, offset = 1, nodes - 1
    while offset > 0:
        count *= 2
        offset -= count
        parent = [below(node_maps[offset + j], j) for j in range(count)]
    for i in range(2 * half):
        full = below(maps_a[i] if i < half else maps_b[i - half], i)
        const[i] = full[:, :cols]
        coef[i] = jnp.concatenate(split(full[:, cols:]), axis=1)


def final_kernel(levels, own, other, const, coef, out, held, sems):
    low = columns_of(levels) == 0
    a, b = own[...], other[...]
    hi, lo = split(
        jnp.concatenate([jnp.where(low, a, b), jnp.where(low, b, a)], axis=0)
    )
    cols = hi.shape[0]
    g = jnp.concatenate(
        [
            jnp.concatenate([hi, hi], axis=1),
            jnp.concatenate([lo, jnp.zeros_like(lo)], axis=1),
        ],
        axis=0,
    )
    copies = []
    for i in range(out.shape[0]):
        moved = dot(coef[i], g, 1)
        held[i] = const[i] + (moved[:, :cols] + moved[:, cols:])
        copies.append(pltpu.make_async_copy(held.at[i], out.at[i], sems.at[i]))
        copies[i].start()
    for copy in copies:
        copy.wait()


def window_kernel(parts, *refs):
    taken = sum(n_in for _, n_in, _ in parts)
    given = taken
    at = 0
    running = []
    for part, n_in, n_out in parts:
        running.append(part(*refs[at : at + n_in], *refs[given : given + n_out]))
        at += n_in
        given += n_out
    while running:
        running = [job for job in running if next(job, True) is None]


def together(*jobs):
    parts = [(kernel, len(ins), len(outs)) for kernel, outs, ins in jobs]
    outs = [o for _, o, _ in jobs]
    flat = call(
        functools.partial(window_kernel, parts),
        sum(outs, []),
        sum([ins for _, _, ins in jobs], []),
    )
    results = []
    for o in outs:
        results.append(flat[: len(o)])
        flat = flat[len(o) :]
    return results


def swapped(value, mask):
    pairs = [(i, i ^ mask) for i in range(lax.axis_size("leaf"))]
    return lax.ppermute(value, "leaf", pairs)


def body(rhs, leaf_q, leaf_e, leaf_w, node_q, node_e, node_w, top_q, top_e, top_w):
    leaves, size, cols = rhs.shape
    nodes = node_q.shape[0]
    width = leaf_w.shape[2]
    levels = lax.axis_size("leaf").bit_length() - 1
    weights = [leaf_q, leaf_e, leaf_w, node_q, node_e, node_w, top_q, top_e, top_w]
    res = call(
        functools.partial(up_kernel, levels),
        [
            ((cols // 2, width), F32),
            ((cols // 2, width), F32),
            (rhs.shape, F32),
            ((nodes, size, cols), F32),
        ]
        + [(a.shape, F32) for a in weights],
        [rhs] + weights,
        scratch=[pltpu.VMEM(rhs.shape, F32), pltpu.SemaphoreType.DMA((10,))],
        hbm_ins=range(10),
    )
    block, sent, yl, bn, lq, le, lw, nq, ne, nw, tq, te, tw = res

    half = leaves // 2
    plan = {
        2: [(leaf_kernel, 0, half), (node_kernel, nodes - 1, 1)],
        3: [(leaf_kernel, half, half)],
        levels: [(node_kernel, 0, nodes - 1)],
    }
    trans, k, maps = [], [], []
    for level in range(1, levels + 1):
        last = level == levels
        other = swapped(sent if level == 1 else block, 2 ** (level - 1) | 1)
        wide = 2 * width if last else 3 * width
        jobs = [
            (
                functools.partial(level_kernel, level, levels),
                [((size, wide), BF16)] * 2 + ([] if last else [((width, size), F32)]),
                [tq, te, tw] + trans,
            )
        ]
        if level in plan:
            for kernel, begin, count in plan[level]:
                ins = [lq, le, lw, yl] if kernel is leaf_kernel else [nq, ne, nw, bn]
                jobs.append(
                    (
                        functools.partial(kernel, begin),
                        [((count, size, cols + width), F32)],
                        ins + [block],
                    )
                )
        made, *chores = together(*jobs)
        trans = made[2:]
        chores = [c[0] for c in chores]
        maps += chores
        block, k_new = call(
            functools.partial(root_kernel if last else step_kernel, level),
            [((cols // 2, width), F32), ((cols // 2, width if last else size), F32)],
            [made[0], made[1], block, other] + k + chores,
        )
        k = [k_new]
    other = swapped(k[0], 1)
    const, coef = call(
        compose_kernel,
        [((leaves, size, cols), F32), ((leaves, size, 2 * width), BF16)],
        maps + [block],
    )
    return call(
        functools.partial(final_kernel, levels),
        [((leaves, size, cols), F32)],
        [block, other, const, coef],
        scratch=[pltpu.VMEM(rhs.shape, F32), pltpu.SemaphoreType.DMA((leaves,))],
        out_space=pltpu.HBM,
    )[0]


def solution(mesh):
    spec = P(("freq", "leaf"), None, None)
    return jax.shard_map(body, mesh=mesh, in_specs=(spec,) * 10, out_specs=spec, check_vma=False)
```

```python
import functools

import jax
import jax.numpy as jnp
from jax import lax
from jax.experimental import pallas as pl
from jax.experimental.pallas import tpu as pltpu
from jax.sharding import PartitionSpec as P

F32 = jnp.float32
BF16 = jnp.bfloat16


def split(x):
    hi = x.astype(BF16)
    return hi, (x - hi.astype(F32)).astype(BF16)


def dot(a, b, contract=0):
    return lax.dot_general(a, b, (((1,), (contract,)), ((), ())), preferred_element_type=F32)


def mul(a, b):
    left = jnp.concatenate([a[0], a[0], a[1]], axis=1)
    right = jnp.concatenate([b[0], b[1], b[0]], axis=0)
    return dot(left, right)


def mul_narrow(a, b):
    m, n = a[0].shape[0], b[0].shape[1]
    step = 64
    stack = [part[i : i + step] for i in range(0, m, step) for part in a]
    r = dot(jnp.concatenate(stack, axis=0), jnp.concatenate(b, axis=1))
    out = []
    for i in range(0, 2 * m, 2 * step):
        top, low = r[i : i + step], r[i + step : i + 2 * step]
        out.append(top[:, :n] + (top[:, n:] + low[:, :n]))
    return jnp.concatenate(out, axis=0)


def mul_short(a, b):
    m = a[0].shape[0]
    r = dot(jnp.concatenate(a, axis=0), b[0])
    return r[:m] + (r[m:] + dot(a[0], b[1]))


def beside(*pairs):
    return tuple(jnp.concatenate(parts, axis=1) for parts in zip(*pairs))


def call(kernel, outs, ins, scratch=(), hbm_ins=(), out_space=pltpu.VMEM):
    specs = [
        pl.BlockSpec(memory_space=pltpu.HBM if i in hbm_ins else pltpu.VMEM)
        for i in range(len(ins))
    ]
    ins = [
        pltpu.with_memory_space_constraint(x, pltpu.HBM) if i in hbm_ins else x
        for i, x in enumerate(ins)
    ]
    made = pl.pallas_call(
        kernel,
        out_shape=[jax.ShapeDtypeStruct(s, d) for s, d in outs],
        in_specs=specs,
        out_specs=[pl.BlockSpec(memory_space=out_space) for _ in outs],
        scratch_shapes=list(scratch),
        compiler_params=pltpu.CompilerParams(vmem_limit_bytes=24 << 20),
    )(*ins)
    return list(made)


def side_of(level):
    return lax.rem(lax.axis_index("leaf") // 2 ** (level - 1), 2)


def columns_of(levels):
    return lax.rem(sum(side_of(level) for level in range(1, levels + 1)), 2)


def up_kernel(
    levels, rhs, lq, le, lw, nq, ne, nw, tq, te, tw,
    keep, send, yl, bn, lqv, lev, lwv, nqv, nev, nwv, tqv, tev, twv,
    rhsv, sems,
):
    leaves, nodes = rhs.shape[0], nq.shape[0]
    copies = []

    def start(src, dst):
        copy = pltpu.make_async_copy(src, dst, sems.at[len(copies)])
        copy.start()
        copies.append(copy)
        return copy

    got = {}
    got['b'] = start(rhs, rhsv)
    got['q'] = start(lq, lqv)
    got['nw'] = start(nw, nwv)
    got['w'] = start(lw, lwv)
    got['e'] = start(le, lev)
    got['ne'] = start(ne, nev)
    got['nq'] = start(nq, nqv)
    got_top = [start(tq, tqv), start(te, tev), start(tw, twv)]

    got['b'].wait()
    got['q'].wait()
    mid = [split(mul_narrow(split(lqv[i]), split(rhsv[i]))) for i in range(leaves)]
    got['nw'].wait()
    got['w'].wait()
    got['e'].wait()
    vals = []
    for i in range(leaves):
        y = mul_narrow(split(lev[i]), mid[i])
        yl[i] = y
        vals.append(split(y))
    node_wt = [split(nwv[i].T) for i in range(nodes)]
    leaf_wt = [split(lwv[i].T) for i in range(leaves)]
    got['ne'].wait()
    got['nq'].wait()
    half_maps = [split(mul(node_wt[i], split(nev[i]))) for i in range(nodes)]
    reduced = [mul_narrow(leaf_wt[i], vals[i]) for i in range(leaves)]
    maps = [split(mul(half_maps[i], split(nqv[i]))) for i in range(nodes)]
    offset = 0
    while len(reduced) > 1:
        count = len(reduced) // 2
        b = [jnp.concatenate(reduced[2 * j : 2 * j + 2], axis=0) for j in range(count)]
        for j in range(count):
            bn[offset + j] = b[j]
        reduced = [mul_narrow(maps[offset + j], split(b[j])) for j in range(count)]
        offset += count
    c = reduced[0].T
    half = c.shape[0] // 2
    low = columns_of(levels) == 0
    keep[...] = jnp.where(low, c[:half], c[half:])
    send[...] = jnp.where(low, c[half:], c[:half])
    for copy in got_top:
        copy.wait()


def level_kernel(level, levels, tq, te, tw, *refs):
    first, last = level == 1, level == levels
    outs = refs if first else refs[2:]
    width = tw.shape[2]
    half = pl.ds(pl.multiple_of(side_of(level) * width, width), width)
    at = level - 1
    if last:
        c = mul(split(te[at, half, :]), split(tq[at])).T
        yield
        if not first:
            c = mul(split(c), split(refs[0][...]))
        outs[0][...], outs[1][...] = split(c)
        yield
        outs[-1][...] = mul_short(split(refs[1][...]), (outs[0][half, :], outs[1][half, :]))
        return
    e, w = split(te[at]), split(tw[at])
    x = mul(e, split(tq[at]))
    z = mul_narrow(e, w)
    yield
    if first:
        q = split(tq[at])
        outs[0][...], outs[1][...] = split(mul(split(x.T), beside(w, q)))
        outs[2][...] = -mul(split(z.T), q)
        return
    q = split(tq[at, :, half])
    both = mul(split(x.T), beside(w, q))
    g = mul_narrow(split(z.T), q)
    yield
    low = mul(split(jnp.concatenate([both[:, width:], g], axis=0)), split(refs[0][...]))
    a = split(both[:, :width])
    tb = split(low[: 2 * width])
    for i in range(2):
        outs[i][:, :width] = a[i]
        outs[i][:, width:] = tb[i]
    outs[2][...] = -low[2 * width :]
    yield
    outs[3][...] = mul_short(split(refs[1][...]), (outs[0][half, :], outs[1][half, :]))


def family(level, own, other):
    right = side_of(level) == 1
    a, b = own[...], other[...]
    return jnp.concatenate([jnp.where(right, b, a), jnp.where(right, a, b)], axis=1)


def product(level, hi, lo, own, other, refs):
    if level == 1:
        return mul_short(split(family(level, own, other)), (hi[...], lo[...]))
    width = own.shape[1]
    far = pl.ds(pl.multiple_of((1 - side_of(level)) * width, width), width)
    return refs[1][...] + mul_short(split(other[...]), (hi[far, :], lo[far, :]))


def step_kernel(level, hi, lo, own, other, *refs):
    width = own.shape[1]
    out = product(level, hi, lo, own, other, refs)
    k = out[:, width:]
    if level > 1:
        k = k + refs[0][...]
    refs[-2][...] = out[:, :width]
    refs[-1][...] = k


def root_kernel(level, hi, lo, own, other, *refs):
    width = own.shape[1]
    x = product(level, hi, lo, own, other, refs)
    if level > 1:
        x = x + refs[0][...]
    right = side_of(1) == 1
    refs[-2][...] = jnp.where(right, x[:, width:], x[:, :width])
    refs[-1][...] = jnp.where(right, x[:, :width], x[:, width:])


def leaf_kernel(begin, q, e, w, y, after, out):
    run = range(out.shape[0])
    ew = [split(mul_narrow(split(e[begin + i]), split(w[begin + i]))) for i in run]
    yield
    for i in run:
        out[i] = mul(split(q[begin + i].T), beside(split(y[begin + i]), ew[i]))


def node_kernel(begin, q, e, w, b, after, out):
    run = range(out.shape[0])
    t = [split(mul_narrow(split(q[begin + i]), split(b[begin + i]))) for i in run]
    yield
    y_ew = [split(mul(split(e[begin + i]), beside(t[i], split(w[begin + i])))) for i in run]
    yield
    for i in run:
        out[i] = mul(split(q[begin + i].T), y_ew[i])


def compose_kernel(maps_a, root_map, maps_b, node_maps, after, const, coef):
    nodes = node_maps.shape[0] + 1
    half = maps_a.shape[0]
    cols = const.shape[2]
    width = maps_a.shape[2] - cols
    top = root_map[0]
    parent = [jnp.concatenate([top[:, :cols], -top[:, cols:]], axis=1)]

    def below(vg, j):
        block = split(parent[j // 2][j % 2 * width : (j % 2 + 1) * width])
        moved = mul(split(vg[:, cols:]), block)
        return jnp.concatenate([vg[:, :cols] - moved[:, :cols], -moved[:, cols:]], axis=1)

    count, offset = 1, nodes - 1
    while offset > 0:
        count *= 2
        offset -= count
        parent = [below(node_maps[offset + j], j) for j in range(count)]
    for i in range(2 * half):
        full = below(maps_a[i] if i < half else maps_b[i - half], i)
        const[i] = full[:, :cols]
        coef[i] = jnp.concatenate(split(full[:, cols:]), axis=1)


def final_kernel(levels, own, other, const, coef, out, held, sems):
    low = columns_of(levels) == 0
    a, b = own[...], other[...]
    hi, lo = split(
        jnp.concatenate([jnp.where(low, a, b), jnp.where(low, b, a)], axis=0)
    )
    cols = hi.shape[0]
    g = jnp.concatenate(
        [
            jnp.concatenate([hi, hi], axis=1),
            jnp.concatenate([lo, jnp.zeros_like(lo)], axis=1),
        ],
        axis=0,
    )
    copies = []
    for i in range(out.shape[0]):
        moved = dot(coef[i], g, 1)
        held[i] = const[i] + (moved[:, :cols] + moved[:, cols:])
        copies.append(pltpu.make_async_copy(held.at[i], out.at[i], sems.at[i]))
        copies[i].start()
    for copy in copies:
        copy.wait()


def window_kernel(parts, *refs):
    taken = sum(n_in for _, n_in, _ in parts)
    given = taken
    at = 0
    running = []
    for part, n_in, n_out in parts:
        running.append(part(*refs[at : at + n_in], *refs[given : given + n_out]))
        at += n_in
        given += n_out
    while running:
        running = [job for job in running if next(job, True) is None]


def together(*jobs):
    parts = [(kernel, len(ins), len(outs)) for kernel, outs, ins in jobs]
    outs = [o for _, o, _ in jobs]
    flat = call(
        functools.partial(window_kernel, parts),
        sum(outs, []),
        sum([ins for _, _, ins in jobs], []),
    )
    results = []
    for o in outs:
        results.append(flat[: len(o)])
        flat = flat[len(o) :]
    return results


def swapped(value, mask):
    pairs = [(i, i ^ mask) for i in range(lax.axis_size("leaf"))]
    return lax.ppermute(value, "leaf", pairs)


def body(rhs, leaf_q, leaf_e, leaf_w, node_q, node_e, node_w, top_q, top_e, top_w):
    leaves, size, cols = rhs.shape
    nodes = node_q.shape[0]
    width = leaf_w.shape[2]
    levels = lax.axis_size("leaf").bit_length() - 1
    weights = [leaf_q, leaf_e, leaf_w, node_q, node_e, node_w, top_q, top_e, top_w]
    res = call(
        functools.partial(up_kernel, levels),
        [
            ((cols // 2, width), F32),
            ((cols // 2, width), F32),
            (rhs.shape, F32),
            ((nodes, size, cols), F32),
        ]
        + [(a.shape, F32) for a in weights],
        [rhs] + weights,
        scratch=[pltpu.VMEM(rhs.shape, F32), pltpu.SemaphoreType.DMA((10,))],
        hbm_ins=range(10),
    )
    block, sent, yl, bn, lq, le, lw, nq, ne, nw, tq, te, tw = res

    half = leaves // 2
    plan = {
        2: [(leaf_kernel, 0, half), (node_kernel, nodes - 1, 1)],
        3: [(leaf_kernel, half, half)],
        levels: [(node_kernel, 0, nodes - 1)],
    }
    trans, k, maps = [], [], []
    for level in range(1, levels + 1):
        last = level == levels
        other = swapped(sent if level == 1 else block, 2 ** (level - 1) | 1)
        wide = 2 * width if last else 3 * width
        jobs = [
            (
                functools.partial(level_kernel, level, levels),
                [((size, wide), BF16)] * 2
                + ([] if last else [((width, size), F32)])
                + ([] if level == 1 else [((cols // 2, wide), F32)]),
                [tq, te, tw] + trans + ([] if level == 1 else [block]),
            )
        ]
        if level in plan:
            for kernel, begin, count in plan[level]:
                ins = [lq, le, lw, yl] if kernel is leaf_kernel else [nq, ne, nw, bn]
                jobs.append(
                    (
                        functools.partial(kernel, begin),
                        [((count, size, cols + width), F32)],
                        ins + [block],
                    )
                )
        made, *chores = together(*jobs)
        trans, part = made[2:3], made[-1:] if level > 1 else []
        chores = [c[0] for c in chores]
        maps += chores
        block, k_new = call(
            functools.partial(root_kernel if last else step_kernel, level),
            [((cols // 2, width), F32), ((cols // 2, width if last else size), F32)],
            [made[0], made[1], block, other] + k + part + chores,
        )
        k = [k_new]
    other = swapped(k[0], 1)
    const, coef = call(
        compose_kernel,
        [((leaves, size, cols), F32), ((leaves, size, 2 * width), BF16)],
        maps + [block],
    )
    return call(
        functools.partial(final_kernel, levels),
        [((leaves, size, cols), F32)],
        [block, other, const, coef],
        scratch=[pltpu.VMEM(rhs.shape, F32), pltpu.SemaphoreType.DMA((leaves,))],
        out_space=pltpu.HBM,
    )[0]


def solution(mesh):
    spec = P(("freq", "leaf"), None, None)
    return jax.shard_map(body, mesh=mesh, in_specs=(spec,) * 10, out_specs=spec, check_vma=False)
```
